32 devices in a mesh: blk: 4 (over z), team: 4 (over y, core), heads: 2 (over x).
Axes of the slice: x: 2, y: 2, z: 4, core: 2. Of those that a mesh axis runs over, the one named last changes fastest.
Arguments:
- queries: bfloat16 [512, 1024], P('blk', ('team', 'heads')), may hold values from -16 to 16
- keys: bfloat16 [512, 256], P(('blk', 'team'), 'heads'), may hold values from -16 to 16
- values: bfloat16 [512, 256], P(('blk', 'team'), 'heads'), may hold values from -6 to 6
- out_grads: bfloat16 [512, 1024], P('blk', ('team', 'heads')), may hold values from -6 to 6
- positions: int32 [512], P('blk'), may hold values from 0 to 511, as said below
Outputs:
- query_grad: bfloat16 [512, 1024], P('blk', ('team', 'heads'))
- key_grad: bfloat16 [512, 256], P(('blk', 'team'), 'heads')
- value_grad: bfloat16 [512, 256], P(('blk', 'team'), 'heads')
The draws below stay inside these ranges and needn't reach their ends.
Inputs may be any that keep to these rules, and one draw needn't show every extreme that they name: positions hold every number of 0 to 511 once; every aligned run of 32 rows holds 32 consecutive rising positions.
All inputs are finite; a program needn't handle non-finite values.
Results may differ from the reference program's by a relative error of at most 0.0069.
Values may be sent and summed in bfloat16 or wider, within the bound.
A program may use at most 64 MiB of HBM per device.

```python
import math
import jax
import jax.numpy as jnp
from jax import lax

HD = 128
PIECE = 32
KV_HEADS = 2
QUERY_HEADS = 8
TOKENS = 512


def draw_queries(key, part):
    base_draw = jnp.clip(jax.random.normal(jax.random.fold_in(key, 21), (TOKENS, QUERY_HEADS * HD), jnp.float32), -6.0, 6.0)
    return base_draw.astype(jnp.bfloat16)


def draw_keys(key, part):
    base_draw = jnp.clip(jax.random.normal(jax.random.fold_in(key, 22), (TOKENS, KV_HEADS * HD), jnp.float32), -6.0, 6.0)
    return base_draw.astype(jnp.bfloat16)


def draw_positions(key, part):
    piece_order = jax.random.permutation(jax.random.fold_in(key, 11), TOKENS // PIECE)
    placed = piece_order[:, None] * PIECE + jnp.arange(PIECE)[None, :]
    return placed.reshape(-1).astype(jnp.int32)


def block_scale(rng, extent, cuts, smallest, top_value):
    gain, own = 1.0, jax.random.fold_in(rng, 6)
    for axis_at, shards_of in cuts:
        draws = jnp.exp(jax.random.uniform(jax.random.fold_in(own, axis_at), (shards_of,), jnp.float32, smallest / len(cuts), top_value / len(cuts)))
        gain = gain * jnp.repeat(draws, extent[axis_at] // shards_of).reshape([-1 if axis == axis_at else 1 for axis in range(len(extent))])
    return gain


def bell_draw(rng, extent, spread, bound, split=(), kind=jnp.bfloat16):
    drawn = spread * jax.random.normal(rng, extent, jnp.float32)
    if split:
        drawn = drawn * block_scale(rng, extent, split, -0.22, 0.18)
    return jnp.clip(drawn, -bound, bound).astype(kind)


def setup_inputs(seed: int = 0) -> dict:
    seeds = jax.random.split(jax.random.key(seed), 6)
    return {
        "queries": draw_queries(jax.random.fold_in(seeds[5], 71), 0),
        "keys": draw_keys(jax.random.fold_in(seeds[5], 71), 0),
        "values": bell_draw(seeds[2], (TOKENS, KV_HEADS * HD), 1.0, 6.0, ((0, 16), (1, 2))),
        "out_grads": bell_draw(seeds[3], (TOKENS, QUERY_HEADS * HD), 1.0, 6.0, ((0, 4), (1, 8))),
        "positions": draw_positions(jax.random.fold_in(seeds[5], 71), 0),
    }


masked_score = -1e+30

def block_scores(query_block, grad_block, place_block, keys, values, key_places):
    head_dim = keys.shape[1]
    scale = 1.0 / math.sqrt(head_dim)
    row_count = query_block.shape[0]
    query_flat = query_block.reshape(-1, head_dim)
    grad_flat = grad_block.reshape(-1, head_dim)
    scores = jnp.dot(query_flat, keys.T, preferred_element_type=jnp.float32) * scale
    scores = scores.reshape(row_count, -1, keys.shape[0])
    visible = place_block[:, None, None] >= key_places[None, None, :]
    scores = jnp.where(visible, scores, masked_score)
    products = jnp.dot(grad_flat, values.T, preferred_element_type=jnp.float32).reshape(scores.shape)
    return (scores, products, visible)

def one_group(queries, keys, values, out_grads, places):
    head_dim = keys.shape[1]
    total = queries.shape[0]
    scale = 1.0 / math.sqrt(head_dim)
    block_rows = math.gcd(total, 128)
    blocks = total // block_rows
    query_blocks = queries.reshape(blocks, block_rows, -1, head_dim)
    grad_blocks = out_grads.reshape(blocks, block_rows, -1, head_dim)
    place_blocks = places.reshape(blocks, block_rows)

    def statistics(inputs):
        query_block, grad_block, place_block = inputs
        scores, products, visible = block_scores(query_block, grad_block, place_block, keys, values, places)
        maxima = lax.optimization_barrier(jnp.max(scores, axis=-1))
        weights = jnp.where(visible, jnp.exp(scores - maxima[..., None]), 0.0)
        totals = lax.optimization_barrier(jnp.sum(weights, axis=-1))
        traces = lax.optimization_barrier(jnp.sum(weights * products, axis=-1))
        return (maxima + jnp.log(totals), traces / totals)
    lse_all, delta_all = lax.map(statistics, (query_blocks, grad_blocks, place_blocks))

    def backward(sums_state, inputs):
        key_sum, value_sum = sums_state
        query_block, grad_block, place_block, lse_block, delta_block = inputs
        scores, products, visible = block_scores(query_block, grad_block, place_block, keys, values, places)
        weights = jnp.where(visible, jnp.exp(scores - lse_block[..., None]), 0.0)
        rounded = weights.astype(jnp.bfloat16).reshape(-1, total)
        slopes = (weights * (products - delta_block[..., None])).astype(jnp.bfloat16).reshape(-1, total)
        value_sum = value_sum + jnp.dot(rounded.T, grad_block.reshape(-1, head_dim), preferred_element_type=jnp.float32)
        key_sum = key_sum + jnp.dot(slopes.T, query_block.reshape(-1, head_dim), preferred_element_type=jnp.float32) * scale
        query_part = jnp.dot(slopes, keys, preferred_element_type=jnp.float32) * scale
        return ((key_sum, value_sum), query_part.reshape(query_block.shape).astype(jnp.bfloat16))
    zeros = jnp.zeros((total, head_dim), jnp.float32)
    (key_sum, value_sum), query_parts = lax.scan(backward, (zeros, zeros), (query_blocks, grad_blocks, place_blocks, lse_all, delta_all))
    return (query_parts.reshape(total, -1, head_dim), key_sum.astype(jnp.bfloat16), value_sum.astype(jnp.bfloat16))

def reference(queries, keys, values, out_grads, positions):
    total = queries.shape[0]
    head_dim = HD
    group_count = KV_HEADS
    places = positions.astype(jnp.float32)
    query_four = queries.reshape(total, -1, group_count, head_dim)
    grad_four = out_grads.reshape(total, -1, group_count, head_dim)
    query_list = []
    key_list = []
    value_list = []
    for group in range(group_count):
        keys_here = keys[:, group * head_dim:(group + 1) * head_dim]
        values_here = values[:, group * head_dim:(group + 1) * head_dim]
        query_part, key_part, value_part = one_group(query_four[:, :, group, :], keys_here, values_here, grad_four[:, :, group, :], places)
        query_list.append(query_part)
        key_list.append(key_part)
        value_list.append(value_part)
    query_grad = jnp.stack(query_list, 2).reshape(queries.shape)
    return (query_grad, jnp.concatenate(key_list, 1), jnp.concatenate(value_list, 1))
```

```python
import functools
import math

import jax
import jax.numpy as jnp
from jax import lax
from jax.experimental import pallas as pl
from jax.experimental.pallas import tpu as pltpu
from jax.sharding import PartitionSpec as P

masked_score = -1e30
MESH = pl.DeviceIdType.MESH


def contract_last(left, right):
    return lax.dot_general(
        left, right, (((1,), (1,)), ((), ())), preferred_element_type=jnp.float32
    )


def contract_first(left, right):
    return lax.dot_general(
        left, right, (((0,), (0,)), ((), ())), preferred_element_type=jnp.float32
    )


def each(count, body):
    if count <= 16:
        for index in range(count):
            body(index)
    else:

        def step(index, carry):
            body(index)
            return carry

        lax.fori_loop(0, count, step, 0)


def fold(count, body, init):
    if count <= 16:
        for index in range(count):
            init = body(index, init)
        return init
    return lax.fori_loop(0, count, body, init)


def join_rows(pieces):
    count, rows, width = pieces.shape
    if rows % 16:
        return pieces.astype(jnp.float32).reshape(count * rows, width).astype(pieces.dtype)
    return pieces.reshape(count * rows, width)


def kernel(
    blocks,
    team,
    q_hbm,
    k_hbm,
    v_hbm,
    g_hbm,
    p_hbm,
    qg_ref,
    kg_ref,
    vg_ref,
    q_ref,
    g_ref,
    p_ref,
    own,
    kv,
    start,
    starts,
    scores,
    products,
    slopes_ref,
    tops,
    stats,
    stats_in,
    query_sums,
    query_in,
    parts,
    landed,
    load_sem,
    own_send,
    own_recv,
    start_send,
    start_recv,
    head_send,
    head_recv,
    stat_send,
    stat_recv,
    part_send,
    part_recv,
    query_send,
    query_recv,
):
    my_blk, my_team = lax.axis_index("blk"), lax.axis_index("team")
    rows, head_dim = q_ref.shape[1:]
    piece = k_hbm.shape[0]
    scale = 1.0 / math.sqrt(head_dim)
    half = team // 2
    count = blocks * half
    side = lax.rem(my_team, 2)
    other = 1 - side
    my_slot = my_blk * half + lax.div(my_team, 2)
    twin = {"blk": my_blk, "team": my_team + 1 - 2 * side}

    def peer_at(slot):
        slot = jnp.int32(slot)
        return {
            "blk": lax.div(slot, jnp.int32(half)),
            "team": 2 * lax.rem(slot, jnp.int32(half)) + other,
        }

    def send(src, dst, send_sem, recv_sem, peer):
        pltpu.make_async_remote_copy(
            src_ref=src,
            dst_ref=dst,
            send_sem=send_sem,
            recv_sem=recv_sem,
            device_id=peer,
            device_id_type=MESH,
        ).start()

    def wait_bytes(ref, sem):
        pltpu.make_async_copy(ref, ref, sem).wait()

    barrier = pltpu.get_barrier_semaphore()
    each(
        count,
        lambda slot: pl.semaphore_signal(
            barrier, inc=1, device_id=peer_at(slot), device_id_type=MESH
        ),
    )

    loads = [
        pltpu.make_async_copy(k_hbm, own.at[0], load_sem.at[0]),
        pltpu.make_async_copy(v_hbm, own.at[1], load_sem.at[1]),
        pltpu.make_async_copy(p_hbm, p_ref, load_sem.at[2]),
        pltpu.make_async_copy(q_hbm, q_ref.at[side], load_sem.at[3]),
        pltpu.make_async_copy(g_hbm, g_ref.at[side], load_sem.at[4]),
    ]
    for load in loads:
        load.start()
    loads[2].wait()
    place = p_ref[...].astype(jnp.float32)
    lane = lax.broadcasted_iota(jnp.int32, (1, rows), 1)
    first = jnp.sum(jnp.where(lane == my_team * piece, place, 0.0), axis=1, keepdims=True)
    start[...] = jnp.broadcast_to(first, (1, 2 * rows))
    place_row = jnp.concatenate([place, place], axis=1)
    for which in (0, 1, 3, 4):
        loads[which].wait()
    pl.semaphore_wait(barrier, count)

    def send_own(index):
        peer = peer_at(count - 1 - index)
        send(own, kv.at[my_slot], own_send, own_recv.at[my_blk], peer)

    def send_start(index):
        peer = peer_at(count - 1 - index)
        send(start, starts.at[my_slot], start_send, start_recv, peer)

    each(count, send_own)
    send(q_ref.at[side], q_ref.at[side], head_send, head_recv, twin)
    send(g_ref.at[side], g_ref.at[side], head_send, head_recv, twin)
    each(count, send_start)

    def group(blk_now):
        return pl.ds(blk_now * half, half)

    def block_keys(blk_now, which):
        return join_rows(kv[group(blk_now), which])

    wait_bytes(q_ref, head_recv)
    wait_bytes(starts, start_recv)
    queries = join_rows(q_ref[...])
    grads = join_rows(g_ref[...])
    depth = lax.broadcasted_iota(jnp.int32, (1, piece, 2 * rows), 1).astype(jnp.float32)

    def score_block(index, state):
        top, total, trace = state
        blk_now = blocks - 1 - index
        wait_bytes(kv.at[pl.ds(0, half)], own_recv.at[blk_now])
        found = contract_last(block_keys(blk_now, 0), queries) * scale
        block_products = contract_last(block_keys(blk_now, 1), grads)
        visible = place_row.reshape(1, 1, 2 * rows) - starts[group(blk_now)] >= depth
        masked = jnp.where(visible, found.reshape(half, piece, 2 * rows), masked_score)
        masked = masked.reshape(half * piece, 2 * rows)
        updated = jnp.maximum(top, jnp.max(masked, axis=0, keepdims=True))
        weights = jnp.exp(masked - updated)
        scores[blk_now] = weights
        products[blk_now] = block_products
        tops[blk_now] = updated
        factor = jnp.exp(top - updated)
        total = total * factor + jnp.sum(weights, axis=0, keepdims=True)
        trace = trace * factor + jnp.sum(weights * block_products, axis=0, keepdims=True)
        return updated, total, trace

    nought = jnp.zeros((1, 2 * rows), jnp.float32)
    state = (jnp.full((1, 2 * rows), masked_score, jnp.float32), nought, nought)
    near_top, near_total, near_trace = fold(blocks, score_block, state)
    stats[0], stats[1], stats[2] = near_top, near_total, near_trace
    send(stats, stats_in, stat_send, stat_recv, twin)
    wait_bytes(stats_in, stat_recv)
    far_top, far_total, far_trace = stats_in[0], stats_in[1], stats_in[2]
    top = jnp.maximum(near_top, far_top)
    near_factor, far_factor = jnp.exp(near_top - top), jnp.exp(far_top - top)
    inverse = 1.0 / (near_total * near_factor + far_total * far_factor)
    delta = (near_trace * near_factor + far_trace * far_factor) * inverse

    def grad_block(blk_now):
        weights = scores[blk_now] * (inverse * jnp.exp(tops[blk_now] - top))
        rounded = weights.astype(jnp.bfloat16)
        slopes = (weights * (products[blk_now] - delta)).astype(jnp.bfloat16)
        slopes_ref[blk_now] = slopes
        key_part = jnp.dot(slopes, queries, preferred_element_type=jnp.float32) * scale
        value_part = jnp.dot(rounded, grads, preferred_element_type=jnp.float32)
        slots = group(blk_now)
        parts[slots, 0] = key_part.reshape(half, piece, head_dim).astype(jnp.bfloat16)
        parts[slots, 1] = value_part.reshape(half, piece, head_dim).astype(jnp.bfloat16)

        def send_part(index):
            slot = blk_now * half + index
            send(
                parts.at[slot],
                landed.at[my_slot],
                part_send,
                part_recv.at[my_blk],
                peer_at(slot),
            )

        each(half, send_part)

    each(blocks, grad_block)

    def add_query(blk_now, query_sum):
        return query_sum + contract_first(slopes_ref[blk_now], block_keys(blk_now, 0))

    query_sum = fold(blocks, add_query, jnp.zeros((2 * rows, head_dim), jnp.float32))
    query_sums[...] = query_sum.reshape(2, rows, head_dim)
    send(query_sums.at[other], query_in, query_send, query_recv, twin)
    wait_bytes(q_ref, head_send)
    wait_bytes(kv, own_send)
    wait_bytes(starts, start_send)
    wait_bytes(stats, stat_send)
    wait_bytes(query_in, query_recv)
    qg_ref[...] = ((query_sums[side] + query_in[...]) * scale).astype(jnp.bfloat16)

    def add_landed(blk_now, sums):
        wait_bytes(landed.at[pl.ds(0, half)], part_recv.at[blk_now])

        def add_one(index, sums):
            return sums + landed[blk_now * half + index].astype(jnp.float32)

        return fold(half, add_one, sums)

    sums = fold(blocks, add_landed, jnp.zeros((2, piece, head_dim), jnp.float32))
    kg_ref[...] = sums[0].astype(jnp.bfloat16)
    vg_ref[...] = sums[1].astype(jnp.bfloat16)
    wait_bytes(query_in, query_send)
    wait_bytes(parts, part_send)


def put_out(*refs):
    count = (len(refs) - 1) // 2
    copies = [
        pltpu.make_async_copy(refs[i], refs[count + i], refs[-1].at[i]) for i in range(count)
    ]
    for copy in copies:
        copy.start()
    for copy in copies:
        copy.wait()


def per_device(queries, keys, values, out_grads, positions):
    blocks, team = lax.axis_size("blk"), lax.axis_size("team")
    half = team // 2
    count = blocks * half
    rows, head_dim = queries.shape
    piece = keys.shape[0]
    any_space = pl.BlockSpec(memory_space=pl.ANY)
    near_space = pl.BlockSpec(memory_space=pltpu.VMEM)
    results = (queries, keys, values)
    one = pltpu.SemaphoreType.DMA
    many = pltpu.SemaphoreType.DMA((blocks,))
    heads = pltpu.VMEM((2, rows, head_dim), jnp.bfloat16)
    slots = pltpu.VMEM((count, 2, piece, head_dim), jnp.bfloat16)
    square = pltpu.VMEM((blocks, half * piece, 2 * rows), jnp.float32)
    held = pl.pallas_call(
        functools.partial(kernel, blocks, team),
        out_shape=tuple(pltpu.VMEM(one.shape, jnp.bfloat16) for one in results),
        in_specs=[any_space] * 5,
        out_specs=(near_space,) * 3,
        scratch_shapes=[
            heads,
            heads,
            pltpu.VMEM((1, rows), jnp.int32),
            pltpu.VMEM((2, piece, head_dim), jnp.bfloat16),
            slots,
            pltpu.VMEM((1, 2 * rows), jnp.float32),
            pltpu.VMEM((count, 1, 2 * rows), jnp.float32),
            square,
            square,
            pltpu.VMEM((blocks, half * piece, 2 * rows), jnp.bfloat16),
            pltpu.VMEM((blocks, 1, 2 * rows), jnp.float32),
            pltpu.VMEM((3, 1, 2 * rows), jnp.float32),
            pltpu.VMEM((3, 1, 2 * rows), jnp.float32),
            pltpu.VMEM((2, rows, head_dim), jnp.float32),
            pltpu.VMEM((rows, head_dim), jnp.float32),
            slots,
            slots,
            pltpu.SemaphoreType.DMA((5,)),
            one,
            many,
            one,
            one,
            one,
            one,
            one,
            one,
            one,
            many,
            one,
            one,
        ],
        compiler_params=pltpu.CompilerParams(collective_id=0, has_side_effects=True),
    )(queries, keys, values, out_grads, positions.reshape(1, rows))
    return pl.pallas_call(
        put_out,
        out_shape=tuple(jax.ShapeDtypeStruct(one.shape, jnp.bfloat16) for one in results),
        in_specs=[near_space] * 3,
        out_specs=(any_space,) * 3,
        scratch_shapes=[pltpu.SemaphoreType.DMA((3,))],
    )(*(pltpu.with_memory_space_constraint(one, pltpu.VMEM) for one in held))


def solution(mesh):
    in_specs = (
        P("blk", ("team", "heads")),
        P(("blk", "team"), "heads"),
        P(("blk", "team"), "heads"),
        P("blk", ("team", "heads")),
        P("blk"),
    )
    out_specs = (
        P("blk", ("team", "heads")),
        P(("blk", "team"), "heads"),
        P(("blk", "team"), "heads"),
    )
    return jax.shard_map(
        per_device, mesh=mesh, in_specs=in_specs, out_specs=out_specs, check_vma=False
    )
```
